32 devices in a mesh: group: 2 (over y), tm: 4 (over z), bl: 2 (over x), pol: 2 (over core).
Axes of the slice: x: 2, y: 2, z: 4, core: 2. Of those that a mesh axis runs over, the one named last changes fastest.
Arguments:
- visibilities: bfloat16 [1600, 256, 2, 384], P(('group', 'tm'), ('bl', 'pol')), parts along dimension 0, may hold values from -6 to 6
- flag_mask: int32 [1600], P(('group', 'tm')), parts along dimension 0, may hold values 0 or 1
- kernel_index: int32 [256], P(('bl', 'pol')), may hold values from 0 to 15
- filter_bank: float32 [2, 16, 257], replicated, may hold values from -0.875 to 0.875
Outputs:
- fringe_filtered: bfloat16 [160, 256, 2, 384], P('group', ('bl', 'pol', 'tm')), parts along dimension 0
The draws below stay inside these ranges and needn't reach their ends.
There are 2 independent parts, one for each index of `group`. The reference program is written for one: setup_inputs(seed, part) draws one part's arguments, and reference() takes and returns one part's arrays. A program takes and returns all parts, laid end to end along the dimension named above; an argument that names none is the same for every part. Nothing has to cross between parts.
All inputs are finite; a program needn't handle non-finite values. No bound on the sum of `flag_mask` on one device may be relied on, other than what follows from the above.
Results may differ from the reference program's by a relative error of at most 0.001.
Values may be sent and summed in bfloat16 or wider, within the bound.
No kernel may reach another device: no remote copies, remote signals or barrier semaphores. Data moves between devices by JAX's collectives and lax.ppermute only.
A program may use at most 192 MiB of HBM per device.

```python
import jax
import jax.numpy as jnp
from jax import lax

BASE = 256
CHAN = 384
TAPS = 257
AVG = 10
NKERN = 16
T_DEV = 200
TIMES = 800
OUT_TIMES = 80


def place_ends(array, stream_key, least, top_value):
    index_at = [jax.random.randint(jax.random.fold_in(stream_key, axis), (), 0, length) for axis, length in enumerate(array.shape)]
    widest = array.shape.index(max(array.shape))
    neighbour = index_at[:widest] + [(index_at[widest] + 1) % array.shape[widest]] + index_at[widest + 1:]
    return array.at[tuple(index_at)].set(least).at[tuple(neighbour)].set(top_value)


def block_levels(own_key, shape, shards, smallest, largest):
    level, own = 1.0, jax.random.fold_in(own_key, 6)
    for position, shards_of in shards:
        draws = jnp.exp(jax.random.uniform(jax.random.fold_in(own, position), (shards_of,), jnp.float32, smallest / len(shards), largest / len(shards)))
        level = level * jnp.repeat(draws, shape[position] // shards_of).reshape([-1 if axis == position else 1 for axis in range(len(shape))])
    return level


def gaussian(own_key, shape, scale, limit, pieces=(), kind=jnp.bfloat16):
    factor_of = block_levels(own_key, shape, pieces, -0.22, 0.18) if pieces else 1.0
    entries = jax.random.normal(own_key, shape, jnp.float32) * scale * factor_of
    return jnp.minimum(jnp.maximum(entries, -limit), limit).astype(kind)


def setup_inputs(seed: int = 0, part: int = 0) -> dict:
    keys = jax.random.split(jax.random.key(seed), 5)
    part_splits = jax.random.split(jax.random.fold_in(keys[4], part), 5)
    visibilities = gaussian(part_splits[0], (TIMES, BASE, 2, CHAN), 1.0, 6.0, ((0, 4), (1, 4)))
    flag_mask = place_ends((jax.random.randint(part_splits[1], (TIMES,), 0, 10) < 9).astype(jnp.int32), jax.random.fold_in(part_splits[1], 1), 0, 1)
    kernel_index = place_ends(jax.random.randint(keys[2], (BASE,), 0, NKERN), jax.random.fold_in(keys[2], 1), 0, NKERN - 1).astype(jnp.int32)
    filter_bank = gaussian(keys[3], (2, NKERN, TAPS), (TAPS // 5) ** -0.5, 0.875, (), jnp.float32)
    return {"visibilities": visibilities, "flag_mask": flag_mask, "kernel_index": kernel_index, "filter_bank": filter_bank}


def select_taps(kernel_index, filter_bank):
    choices_count = filter_bank.shape[1]
    one_hot = (kernel_index[:, None] == jnp.arange(choices_count, dtype=jnp.int32)[None, :]).astype(jnp.float32)
    return jnp.einsum("bk,rkt->brt", one_hot, filter_bank, precision=lax.Precision.HIGHEST)


def make_band(kernel_taps, block_rows):
    tap_count = kernel_taps.shape[1]
    row_width = block_rows + tap_count - 1
    zero_tail = jnp.zeros((2, block_rows), jnp.float32)
    period_row = jnp.concatenate([kernel_taps, zero_tail], axis=1)
    tiled_rows = jnp.tile(period_row, (1, block_rows))[:, :block_rows * row_width]
    return tiled_rows.reshape(2, block_rows, row_width)


def filter_block(time_slab, kernel_taps, block_rows, joined_average):
    band_rows = make_band(kernel_taps, block_rows)
    row_width = band_rows.shape[2]
    if joined_average:
        band_rows = band_rows.reshape(2, block_rows // AVG, AVG, row_width).sum(axis=2) * (1.0 / AVG)
    out_count = band_rows.shape[1]
    stacked = band_rows.reshape(2 * out_count, row_width)
    product = jnp.dot(stacked, time_slab, precision=lax.Precision.HIGHEST, preferred_element_type=jnp.float32)
    prod_real = product[:out_count]
    prod_imag = product[out_count:]
    channels = time_slab.shape[1] // 2
    out_real = prod_real[:, :channels] - prod_imag[:, channels:]
    out_imag = prod_real[:, channels:] + prod_imag[:, :channels]
    result = jnp.stack([out_real, out_imag], axis=1)
    if not joined_average:
        result = result.reshape(out_count // AVG, AVG, 2, channels).sum(axis=1) * (1.0 / AVG)
    return result


def reference(visibilities, flag_mask, kernel_index, filter_bank):
    half_taps = TAPS // 2
    flag_float = flag_mask.astype(jnp.float32)
    taps_all = select_taps(kernel_index, filter_bank)
    block_count = TIMES // T_DEV

    def per_base(base_index):
        column = lax.dynamic_index_in_dim(visibilities, base_index, 1, False).astype(jnp.float32)
        column = (column * flag_float[:, None, None]).reshape(TIMES, 2 * CHAN)
        padded = jnp.pad(column, ((half_taps, half_taps), (0, 0)))
        kernel_taps = lax.dynamic_index_in_dim(taps_all, base_index, 0, False)

        def per_block(block_index):
            time_slab = lax.dynamic_slice_in_dim(padded, (block_index * T_DEV).astype(jnp.int32), T_DEV + TAPS - 1, 0)
            return filter_block(time_slab, kernel_taps, T_DEV, True)

        blocks_out = lax.map(per_block, jnp.arange(block_count, dtype=jnp.int32))
        return blocks_out.reshape(OUT_TIMES, 2, CHAN)

    filtered = lax.map(per_base, jnp.arange(BASE, dtype=jnp.int32))
    return jnp.moveaxis(filtered, 0, 1).astype(jnp.bfloat16)
```

```python
import functools

import jax
import jax.numpy as jnp
from jax import lax
from jax.experimental import pallas as pl
from jax.experimental.pallas import tpu as pltpu
from jax.sharding import PartitionSpec as P

TAPS = 257
AVG = 10
HALF = TAPS // 2
HALO = -(-HALF // AVG)


def round_up(value, step):
    return -(-value // step) * step


def line_pair(filter_bank, rows, lines):
    summed = sum(
        jnp.pad(filter_bank, ((0, 0), (0, 0), (j, AVG - 1 - j))) for j in range(AVG)
    ) * (1.0 / AVG)
    real, imag = summed[0], summed[1]
    pair = jnp.stack(
        [jnp.stack([real, -imag], axis=-1), jnp.stack([imag, real], axis=-1)], axis=1
    )
    pair = pair.reshape(real.shape[0], 2, 2 * real.shape[1])
    period = round_up(2 * rows + 2 * AVG * lines, 128)
    split = 2 * (AVG * HALO + HALF)
    gap = jnp.zeros(pair.shape[:2] + (period - pair.shape[2],), jnp.float32)
    return jnp.concatenate([pair[:, :, split:], gap, pair[:, :, :split]], axis=2)


def bank_body(lines_ref, flags_ref, bank_ref, *, lines, width):
    for part in range(2):
        row = lines_ref[0, part : part + 1, :]
        spread = jnp.broadcast_to(row, (8, row.shape[1]))
        tiles = []
        for tile in range(lines // 8):
            shifted = pltpu.roll(spread, 2 * AVG * 8 * tile, 1)
            shifted = pltpu.roll(shifted, 0, 1, stride=AVG, stride_axis=0)
            tiles.append(pltpu.roll(shifted, 0, 1, stride=AVG, stride_axis=0)[:, :width])
        band = jnp.concatenate(tiles, axis=0)
        band = band * flags_ref[...]
        high = band.astype(jnp.bfloat16)
        low = (band - high.astype(jnp.float32)).astype(jnp.bfloat16)
        bank_ref[0, part * lines : (part + 1) * lines, :] = high
        bank_ref[0, (2 + part) * lines : (3 + part) * lines, :] = low


def main_body(index_ref, vis_ref, bank_ref, out_ref, *, group, half):
    step = pl.program_id(0)
    rows, _, _, chans = vis_ref.shape
    for i in range(group):
        band = bank_ref[index_ref[step * group + i]]
        slab = vis_ref[:, i, :, :].reshape(2 * rows, chans)
        prod = jnp.dot(band, slab, preferred_element_type=jnp.float32)
        out_ref[i] = prod[:half] + prod[half:]


def partial_rows(visibilities, flag_mask, kernel_index, filter_bank):
    rows, bases, _, chans = visibilities.shape
    kernels = filter_bank.shape[1]
    lines = round_up(rows // AVG + 2 * HALO, 8)
    width = 2 * rows
    pairs = line_pair(filter_bank, rows, lines)
    flags = jnp.repeat(flag_mask.astype(jnp.float32), 2)[None, :]
    bank = pl.pallas_call(
        functools.partial(bank_body, lines=lines, width=width),
        grid=(kernels,),
        in_specs=[
            pl.BlockSpec((1, 2, pairs.shape[2]), lambda k: (k, 0, 0)),
            pl.BlockSpec((1, width), lambda k: (0, 0)),
        ],
        out_specs=pl.BlockSpec((1, 4 * lines, width), lambda k: (k, 0, 0)),
        out_shape=jax.ShapeDtypeStruct((kernels, 4 * lines, width), jnp.bfloat16),
        name="bank",
    )(pairs, flags)
    group = 8 if bases % 8 == 0 else 1
    return pl.pallas_call(
        functools.partial(main_body, group=group, half=2 * lines),
        grid_spec=pltpu.PrefetchScalarGridSpec(
            num_scalar_prefetch=1,
            grid=(bases // group,),
            in_specs=[
                pl.BlockSpec((rows, group, 2, chans), lambda g, _: (0, g, 0, 0)),
                pl.BlockSpec(bank.shape, lambda g, _: (0, 0, 0)),
            ],
            out_specs=pl.BlockSpec((group, 2 * lines, chans), lambda g, _: (g, 0, 0)),
        ),
        out_shape=jax.ShapeDtypeStruct((bases, 2 * lines, chans), jnp.float32),
        compiler_params=pltpu.CompilerParams(vmem_limit_bytes=50 * 1024 * 1024),
        name="partials",
    )(kernel_index, visibilities, bank)


def per_device(visibilities, flag_mask, kernel_index, filter_bank):
    rows, bases, _, chans = visibilities.shape
    own = rows // AVG
    prod = partial_rows(visibilities, flag_mask, kernel_index, filter_bank)
    prod = prod.reshape(bases, 2, prod.shape[1] // 2, chans)
    prod = jnp.transpose(prod, (2, 0, 1, 3))
    count = lax.axis_size("tm")
    up = [(i, i + 1) for i in range(count - 1)]
    down = [(i + 1, i) for i in range(count - 1)]
    from_low = lax.ppermute(prod[own + HALO : own + 2 * HALO], "tm", up)
    from_high = lax.ppermute(prod[:HALO], "tm", down)
    total = prod[HALO : HALO + own]
    total = total + jnp.pad(from_low, ((0, own - HALO), (0, 0), (0, 0), (0, 0)))
    total = total + jnp.pad(from_high, ((own - HALO, 0), (0, 0), (0, 0), (0, 0)))
    averaged = total.astype(jnp.bfloat16)
    return lax.all_to_all(averaged, "tm", split_axis=1, concat_axis=0, tiled=True)


def solution(mesh):
    placed = (
        P(("group", "tm"), ("bl", "pol"), None, None),
        P(("group", "tm")),
        P(("bl", "pol")),
        P(),
    )
    return jax.shard_map(
        per_device,
        mesh=mesh,
        in_specs=placed,
        out_specs=P("group", ("bl", "pol", "tm"), None, None),
        check_vma=False,
    )
```

```python
import functools

import jax
import jax.numpy as jnp
from jax import lax
from jax.experimental import pallas as pl
from jax.experimental.pallas import tpu as pltpu
from jax.sharding import PartitionSpec as P

TAPS = 257
AVG = 10
HALF = TAPS // 2
HALO = -(-HALF // AVG)


def round_up(value, step):
    return -(-value // step) * step


def line_pair(filter_bank, rows, lines):
    summed = sum(
        jnp.pad(filter_bank, ((0, 0), (0, 0), (j, AVG - 1 - j))) for j in range(AVG)
    ) * (1.0 / AVG)
    real, imag = summed[0], summed[1]
    pair = jnp.stack(
        [jnp.stack([real, -imag], axis=-1), jnp.stack([imag, real], axis=-1)], axis=1
    )
    pair = pair.reshape(real.shape[0], 2, 2 * real.shape[1])
    period = round_up(2 * rows + 2 * AVG * lines, 128)
    split = 2 * (AVG * HALO + HALF)
    gap = jnp.zeros(pair.shape[:2] + (period - pair.shape[2],), jnp.float32)
    return jnp.concatenate([pair[:, :, split:], gap, pair[:, :, :split]], axis=2)


def bank_body(lines_ref, flags_ref, bank_ref, *, lines, width):
    for k in range(lines_ref.shape[0]):
        for part in range(2):
            row = lines_ref[k, part : part + 1, :]
            spread = jnp.broadcast_to(row, (8, row.shape[1]))
            tiles = []
            for tile in range(lines // 8):
                shifted = pltpu.roll(spread, 2 * AVG * 8 * tile, 1)
                shifted = pltpu.roll(shifted, 0, 1, stride=AVG, stride_axis=0)
                tiles.append(pltpu.roll(shifted, 0, 1, stride=AVG, stride_axis=0)[:, :width])
            band = jnp.concatenate(tiles, axis=0) * flags_ref[...]
            high = band.astype(jnp.bfloat16)
            low = (band - high.astype(jnp.float32)).astype(jnp.bfloat16)
            bank_ref[k, part * lines : (part + 1) * lines, :] = high
            bank_ref[k, (2 + part) * lines : (3 + part) * lines, :] = low


def main_body(index_ref, vis_ref, bank_ref, out_ref, *, group, half, chunks, chunk):
    first = (pl.program_id(0) * chunks + chunk) * group
    rows, _, _, chans = vis_ref.shape
    for i in range(group):
        band = bank_ref[index_ref[first + i]]
        slab = vis_ref[:, i, :, :].reshape(2 * rows, chans)
        prod = jnp.dot(band, slab, preferred_element_type=jnp.float32)
        out_ref[i] = prod[:half] + prod[half:]


def make_bank(flag_mask, filter_bank, rows):
    kernels = filter_bank.shape[1]
    lines = round_up(rows // AVG + 2 * HALO, 8)
    width = 2 * rows
    pairs = line_pair(filter_bank, rows, lines)
    flags = jnp.repeat(flag_mask.astype(jnp.float32), 2)[None, :]
    per_step = 4 if kernels % 4 == 0 else 1
    return pl.pallas_call(
        functools.partial(bank_body, lines=lines, width=width),
        grid=(kernels // per_step,),
        in_specs=[
            pl.BlockSpec((per_step, 2, pairs.shape[2]), lambda k: (k, 0, 0)),
            pl.BlockSpec((1, width), lambda k: (0, 0)),
        ],
        out_specs=pl.BlockSpec((per_step, 4 * lines, width), lambda k: (k, 0, 0)),
        out_shape=jax.ShapeDtypeStruct((kernels, 4 * lines, width), jnp.bfloat16),
        name="bank",
    )(pairs, flags)


def partial_rows(visibilities, kernel_index, bank, owners, chunks, chunk):
    rows, bases, _, chans = visibilities.shape
    group = bases // owners // chunks
    half = bank.shape[1] // 2
    prod = pl.pallas_call(
        functools.partial(main_body, group=group, half=half, chunks=chunks, chunk=chunk),
        grid_spec=pltpu.PrefetchScalarGridSpec(
            num_scalar_prefetch=1,
            grid=(owners,),
            in_specs=[
                pl.BlockSpec((rows, group, 2, chans), lambda g, _: (0, g * chunks + chunk, 0, 0)),
                pl.BlockSpec(bank.shape, lambda g, _: (0, 0, 0)),
            ],
            out_specs=pl.BlockSpec((group, half, chans), lambda g, _: (g, 0, 0)),
        ),
        out_shape=jax.ShapeDtypeStruct((owners * group, half, chans), jnp.float32),
        compiler_params=pltpu.CompilerParams(vmem_limit_bytes=50 * 1024 * 1024),
        name="partials",
    )(kernel_index, visibilities, bank)
    prod = prod.reshape(owners * group, 2, half // 2, chans)
    return jnp.transpose(prod, (2, 0, 1, 3))


def pack(rows):
    top = jnp.max(jnp.abs(rows), axis=(0, 3), keepdims=True)
    power = jnp.floor(jnp.log2(jnp.maximum(top, 1e-30)))
    scaled = (rows * jnp.exp2(-power)).astype(jnp.float16)
    tail = jnp.broadcast_to(power, (1,) + rows.shape[1:]).astype(jnp.float16)
    return jnp.concatenate([scaled, tail], axis=0)


def unpack(packed):
    wide = packed.astype(jnp.float32)
    return wide[:-1] * jnp.exp2(wide[-1:])


def per_device(visibilities, flag_mask, kernel_index, filter_bank):
    rows, bases, _, chans = visibilities.shape
    own = rows // AVG
    count = lax.axis_size("tm")
    chunks = 2 if (bases // count) % 2 == 0 else 1
    up = [(i, i + 1) for i in range(count - 1)]
    down = [(i + 1, i) for i in range(count - 1)]
    bank = make_bank(flag_mask, filter_bank, rows)
    outputs = []
    for chunk in range(chunks):
        prod = partial_rows(visibilities, kernel_index, bank, count, chunks, chunk)
        from_low = unpack(lax.ppermute(pack(prod[own + HALO : own + 2 * HALO]), "tm", up))
        from_high = unpack(lax.ppermute(pack(prod[:HALO]), "tm", down))
        total = prod[HALO : HALO + own]
        total = total + jnp.pad(from_low, ((0, own - HALO), (0, 0), (0, 0), (0, 0)))
        total = total + jnp.pad(from_high, ((own - HALO, 0), (0, 0), (0, 0), (0, 0)))
        averaged = total.astype(jnp.bfloat16)
        outputs.append(lax.all_to_all(averaged, "tm", split_axis=1, concat_axis=0, tiled=True))
    return jnp.concatenate(outputs, axis=1)


def solution(mesh):
    placed = (
        P(("group", "tm"), ("bl", "pol"), None, None),
        P(("group", "tm")),
        P(("bl", "pol")),
        P(),
    )
    return jax.shard_map(
        per_device,
        mesh=mesh,
        in_specs=placed,
        out_specs=P("group", ("bl", "pol", "tm"), None, None),
        check_vma=False,
    )
```

```python
import functools

import jax
import jax.numpy as jnp
from jax import lax
from jax.experimental import pallas as pl
from jax.experimental.pallas import tpu as pltpu
from jax.sharding import PartitionSpec as P

TAPS = 257
AVG = 10
HALF = TAPS // 2
HALO = -(-HALF // AVG)


def round_up(value, step):
    return -(-value // step) * step


def line_pair(filter_bank, rows, lines):
    summed = sum(
        jnp.pad(filter_bank, ((0, 0), (0, 0), (j, AVG - 1 - j))) for j in range(AVG)
    ) * (1.0 / AVG)
    real, imag = summed[0], summed[1]
    pair = jnp.stack(
        [jnp.stack([real, -imag], axis=-1), jnp.stack([imag, real], axis=-1)], axis=1
    )
    pair = pair.reshape(real.shape[0], 2, 2 * real.shape[1])
    period = round_up(2 * rows + 2 * AVG * lines, 128)
    split = 2 * (AVG * HALO + HALF)
    gap = jnp.zeros(pair.shape[:2] + (period - pair.shape[2],), jnp.float32)
    return jnp.concatenate([pair[:, :, split:], gap, pair[:, :, :split]], axis=2)


def bank_body(lines_ref, flags_ref, bank_ref, *, lines, width):
    head = round_up(width, 128)
    tail = round_up(2 * AVG * 8, 128)
    for k in range(lines_ref.shape[0]):
        for part in range(2):
            row = lines_ref[k, part : part + 1, :]
            spread = jnp.broadcast_to(row, (8, row.shape[1]))
            tiles = []
            for tile in range(lines // 8):
                shifted = pltpu.roll(spread, 2 * AVG * 8 * tile, 1)
                shifted = jnp.concatenate([shifted[:, :head], shifted[:, -tail:]], axis=1)
                shifted = pltpu.roll(shifted, 0, 1, stride=AVG, stride_axis=0)
                tiles.append(pltpu.roll(shifted, 0, 1, stride=AVG, stride_axis=0)[:, :width])
            band = jnp.concatenate(tiles, axis=0) * flags_ref[...]
            high = band.astype(jnp.bfloat16)
            low = (band - high.astype(jnp.float32)).astype(jnp.bfloat16)
            bank_ref[k, part * lines : (part + 1) * lines, :] = high
            bank_ref[k, (2 + part) * lines : (3 + part) * lines, :] = low


def main_body(index_ref, vis_ref, bank_ref, out_ref, *, group, half, chunks, chunk):
    first = (pl.program_id(0) * chunks + chunk) * group
    rows, _, _, chans = vis_ref.shape
    for i in range(group):
        band = bank_ref[index_ref[first + i]]
        slab = vis_ref[:, i, :, :].reshape(2 * rows, chans)
        prod = jnp.dot(band, slab, preferred_element_type=jnp.float32)
        out_ref[i] = prod[:half] + prod[half:]


def make_bank(flag_mask, filter_bank, rows):
    kernels = filter_bank.shape[1]
    lines = round_up(rows // AVG + 2 * HALO, 8)
    width = 2 * rows
    pairs = line_pair(filter_bank, rows, lines)
    flags = jnp.repeat(flag_mask.astype(jnp.float32), 2)[None, :]
    per_step = 1
    return pl.pallas_call(
        functools.partial(bank_body, lines=lines, width=width),
        grid=(kernels // per_step,),
        in_specs=[
            pl.BlockSpec((per_step, 2, pairs.shape[2]), lambda k: (k, 0, 0)),
            pl.BlockSpec((1, width), lambda k: (0, 0)),
        ],
        out_specs=pl.BlockSpec((per_step, 4 * lines, width), lambda k: (k, 0, 0)),
        out_shape=jax.ShapeDtypeStruct((kernels, 4 * lines, width), jnp.bfloat16),
        name="bank",
    )(pairs, flags)


def partial_rows(visibilities, kernel_index, bank, owners, chunks, chunk):
    rows, bases, _, chans = visibilities.shape
    group = bases // owners // chunks
    half = bank.shape[1] // 2
    prod = pl.pallas_call(
        functools.partial(main_body, group=group, half=half, chunks=chunks, chunk=chunk),
        grid_spec=pltpu.PrefetchScalarGridSpec(
            num_scalar_prefetch=1,
            grid=(owners,),
            in_specs=[
                pl.BlockSpec((rows, group, 2, chans), lambda g, _: (0, g * chunks + chunk, 0, 0)),
                pl.BlockSpec(bank.shape, lambda g, _: (0, 0, 0)),
            ],
            out_specs=pl.BlockSpec((group, half, chans), lambda g, _: (g, 0, 0)),
        ),
        out_shape=jax.ShapeDtypeStruct((owners * group, half, chans), jnp.float32),
        compiler_params=pltpu.CompilerParams(vmem_limit_bytes=50 * 1024 * 1024),
        name="partials",
    )(kernel_index, visibilities, bank)
    prod = prod.reshape(owners * group, 2, half // 2, chans)
    return jnp.transpose(prod, (2, 0, 1, 3))


def pack(rows):
    top = jnp.max(jnp.abs(rows), axis=(0, 3), keepdims=True)
    power = jnp.floor(jnp.log2(jnp.maximum(top, 1e-30)))
    scaled = (rows * jnp.exp2(-power)).astype(jnp.float16)
    tail = jnp.broadcast_to(power, (1,) + rows.shape[1:]).astype(jnp.float16)
    return jnp.concatenate([scaled, tail], axis=0)


def unpack(packed):
    wide = packed.astype(jnp.float32)
    return wide[:-1] * jnp.exp2(wide[-1:])


def per_device(visibilities, flag_mask, kernel_index, filter_bank):
    rows, bases, _, chans = visibilities.shape
    own = rows // AVG
    count = lax.axis_size("tm")
    chunks = 2 if (bases // count) % 2 == 0 else 1
    up = [(i, i + 1) for i in range(count - 1)]
    down = [(i + 1, i) for i in range(count - 1)]
    bank = make_bank(flag_mask, filter_bank, rows)
    outputs = []
    for chunk in range(chunks):
        prod = partial_rows(visibilities, kernel_index, bank, count, chunks, chunk)
        from_low = unpack(lax.ppermute(pack(prod[own + HALO : own + 2 * HALO]), "tm", up))
        from_high = unpack(lax.ppermute(pack(prod[:HALO]), "tm", down))
        total = prod[HALO : HALO + own]
        total = total + jnp.pad(from_low, ((0, own - HALO), (0, 0), (0, 0), (0, 0)))
        total = total + jnp.pad(from_high, ((own - HALO, 0), (0, 0), (0, 0), (0, 0)))
        averaged = total.astype(jnp.bfloat16)
        outputs.append(lax.all_to_all(averaged, "tm", split_axis=1, concat_axis=0, tiled=True))
    return jnp.concatenate(outputs, axis=1)


def solution(mesh):
    placed = (
        P(("group", "tm"), ("bl", "pol"), None, None),
        P(("group", "tm")),
        P(("bl", "pol")),
        P(),
    )
    return jax.shard_map(
        per_device,
        mesh=mesh,
        in_specs=placed,
        out_specs=P("group", ("bl", "pol", "tm"), None, None),
        check_vma=False,
    )
```
